32 devices in a mesh: ctx: 16 (over z, x, core), shard: 2 (over y).
Axes of the slice: x: 2, y: 2, z: 4, core: 2. Of those that a mesh axis runs over, the one named last changes fastest.
Arguments:
- layer_input: bfloat16 [4096, 1536], P(('ctx', 'shard')), may hold values from -16 to 16
- positions: int32 [4096], replicated, may hold values from 0 to 4095, as said below
- norm_gain_attn: float32 [1536], replicated, may hold values from 0.1 to 1.9
- w_query: bfloat16 [1536, 1536], P('shard'), may hold values from -1 to 1
- key_weight: bfloat16 [1536, 768], P('shard'), may hold values from -1 to 1
- value_weight: bfloat16 [1536, 768], P('shard'), may hold values from -0.15625 to 0.15625
- w_out: bfloat16 [1536, 1536], P('shard'), may hold values from -3.5 to 3.5
- norm_gain_ffn: float32 [1536], replicated, may hold values from 0.1 to 1.9
- w_gate: bfloat16 [1536, 4096], P('shard'), may hold values from -0.15625 to 0.15625
- w_up: bfloat16 [1536, 4096], P('shard'), may hold values from -0.15625 to 0.15625
- w_down: bfloat16 [4096, 1536], P('shard'), may hold values from -0.09375 to 0.09375
- out_cotangent: bfloat16 [4096, 1536], P(('ctx', 'shard')), may hold values from -6 to 6
Outputs:
- layer_output: bfloat16 [4096, 1536], P(('ctx', 'shard'))
- input_grad: bfloat16 [4096, 1536], P(('ctx', 'shard'))
- grad_norm_attn: float32 [1536], P(('ctx', 'shard'))
- grad_query: float32 [1536, 1536], P(('ctx', 'shard'))
- grad_key: float32 [1536, 768], P(('ctx', 'shard'))
- grad_value: float32 [1536, 768], P(('ctx', 'shard'))
- grad_out: float32 [1536, 1536], P(('ctx', 'shard'))
- grad_norm_ffn: float32 [1536], P(('ctx', 'shard'))
- grad_gate: float32 [1536, 4096], P(('ctx', 'shard'))
- grad_up: float32 [1536, 4096], P(('ctx', 'shard'))
- grad_down: float32 [4096, 1536], P(('ctx', 'shard'))
The draws below stay inside these ranges and needn't reach their ends.
Inputs may be any that keep to these rules, and one draw needn't show every extreme that they name: `positions`: every position 0 to 4095 appears once. The sequence is cut into 2 * 16 blocks of 128 / 2 * 2 rows; a permutation drawn per problem gives each ctx index c a pair number k, and the device of ctx index c and shard index s holds in its first 64 rows the s-th part of block k and in the rest the s-th part of block 2 * 16 - 1 - k, each part in increasing order.
All inputs are finite; a program needn't handle non-finite values.
Results may differ from the reference program's by a relative error of at most 0.025.
Values may be sent and summed in bfloat16 or wider, within the bound.
A program may use at most 512 MiB of HBM per device.

```python
import math
import jax
import jax.numpy as jnp
from jax import lax

MODEL_WIDTH = 1536
QUERY_HEADS = 16
SHARED_KV_UNITS = 8
CHANNEL_SPAN = 96
FF = 4096
TOK_DEV = 128
SEQ = 4096
N_CTX = 16
N_SHARD = 2


def draw_positions(key, part):
    order = jax.random.permutation(jax.random.fold_in(key, 11), N_CTX).astype(jnp.int32)
    half_rows = TOK_DEV // 2
    row_index = jnp.arange(N_CTX * N_SHARD * TOK_DEV, dtype=jnp.int32)
    device = row_index // TOK_DEV
    within = row_index % TOK_DEV
    pair_number = order[device // N_SHARD]
    shard_index = device % N_SHARD
    block = jnp.where(within >= half_rows, 2 * N_CTX - 1 - pair_number, pair_number)
    return (block * (half_rows * N_SHARD) + shard_index * half_rows + within % half_rows).astype(jnp.int32)


def random_projection(key, salt, width):
    base = jax.random.truncated_normal(jax.random.fold_in(key, salt), -6.0, 6.0, (MODEL_WIDTH, width), jnp.float32) / math.sqrt(MODEL_WIDTH)
    return base.astype(jnp.bfloat16)


def draw_w_query(key, part):
    return random_projection(key, 202, QUERY_HEADS * CHANNEL_SPAN)


def draw_key_weight(key, part):
    return random_projection(key, 203, SHARED_KV_UNITS * CHANNEL_SPAN)


def draw_layer_input(key, part):
    noise = jax.random.truncated_normal(jax.random.fold_in(key, 204), -6.0, 6.0, (SEQ, MODEL_WIDTH), jnp.float32)
    return noise.astype(jnp.bfloat16)


def level_of(stream_key, dims, cuts, smallest, high):
    def one(axis_at, parts):
        heights = jax.random.uniform(jax.random.fold_in(jax.random.fold_in(stream_key, 6), axis_at), (parts,), jnp.float32, smallest / len(cuts), high / len(cuts))
        return jnp.repeat(jnp.exp(heights), dims[axis_at] // parts).reshape((-1,) + (1,) * (len(dims) - axis_at - 1))

    level = one(*cuts[0])
    for cut in cuts[1:]:
        level = level * one(*cut)
    return level


def gaussian(stream_key, dims, scale, limit, split=(), kind=jnp.bfloat16):
    entries = jax.random.normal(stream_key, dims, jnp.float32) * scale
    if len(split) > 0:
        entries = level_of(stream_key, dims, split, -0.22, 0.18) * entries
    return jnp.clip(entries, min=-limit, max=limit).astype(kind)


def setup_inputs(seed: int = 0) -> dict:
    streams_of = jax.random.split(jax.random.key(seed), 13)
    layer_input = draw_layer_input(jax.random.fold_in(streams_of[12], 71), 0)
    positions = draw_positions(jax.random.fold_in(streams_of[12], 71), 0)
    norm_gain_attn = jnp.clip(1.0 + 0.18 * jax.random.normal(streams_of[2], (MODEL_WIDTH,), jnp.float32), 0.1, 1.9)
    w_query = draw_w_query(jax.random.fold_in(streams_of[12], 71), 0)
    key_weight = draw_key_weight(jax.random.fold_in(streams_of[12], 71), 0)
    value_weight = gaussian(streams_of[5], (MODEL_WIDTH, SHARED_KV_UNITS * CHANNEL_SPAN), MODEL_WIDTH ** -0.5, 0.15625, ((0, 2),))
    w_out = gaussian(streams_of[6], (QUERY_HEADS * CHANNEL_SPAN, MODEL_WIDTH), (max(QUERY_HEADS * CHANNEL_SPAN // 512, 1)) ** -0.5, 3.5, ((0, 2),))
    norm_gain_ffn = jnp.clip(1.0 + 0.18 * jax.random.normal(streams_of[7], (MODEL_WIDTH,), jnp.float32), 0.1, 1.9)
    w_gate = gaussian(streams_of[8], (MODEL_WIDTH, FF), MODEL_WIDTH ** -0.5, 0.15625, ((0, 2),))
    w_up = gaussian(streams_of[9], (MODEL_WIDTH, FF), MODEL_WIDTH ** -0.5, 0.15625, ((0, 2),))
    w_down = gaussian(streams_of[10], (FF, MODEL_WIDTH), FF ** -0.5, 0.09375, ((0, 2),))
    out_cotangent = gaussian(streams_of[11], (SEQ, MODEL_WIDTH), 1.0, 6.0, ((0, 32),))
    return {"layer_input": layer_input, "positions": positions, "norm_gain_attn": norm_gain_attn, "w_query": w_query, "key_weight": key_weight, "value_weight": value_weight, "w_out": w_out, "norm_gain_ffn": norm_gain_ffn, "w_gate": w_gate, "w_up": w_up, "w_down": w_down, "out_cotangent": out_cotangent}


epsilon = 1e-05
rope_base = 100000.0
mask_fill_value = -1e+30

def rope_tables(positions):
    half_size = CHANNEL_SPAN // 2
    frequency = rope_base ** (-2.0 * jnp.arange(half_size, dtype=jnp.float32) / CHANNEL_SPAN)
    angles = positions.astype(jnp.float32)[:, None] * frequency[None, :]
    return (jnp.cos(angles)[:, None, :], jnp.sin(angles)[:, None, :])

def apply_rotary(value_matrix, cosine_table, sine_table):
    half_size = value_matrix.shape[-1] // 2
    first_half = value_matrix[..., :half_size]
    second_half = value_matrix[..., half_size:]
    return jnp.concatenate([first_half * cosine_table - second_half * sine_table, second_half * cosine_table + first_half * sine_table], axis=-1)

def back_project(gradient, weight):
    return lax.dot_general(gradient, weight, (((1,), (1,)), ((), ())), preferred_element_type=jnp.float32)

def weight_grad(inputs, gradient):
    return lax.dot_general(inputs, gradient, (((0,), (0,)), ((), ())), preferred_element_type=jnp.float32)

def rounded_copy(value_matrix):
    return lax.optimization_barrier(value_matrix.astype(jnp.bfloat16)).astype(jnp.float32)

def rms_backward(grad_normed, normed, inverse_rms, gain):
    scaled = grad_normed * gain
    inner = lax.optimization_barrier(jnp.mean(scaled * normed, axis=-1, keepdims=True))
    return (inverse_rms * (scaled - normed * inner), lax.optimization_barrier(jnp.sum(grad_normed * normed, axis=0)))

def reference(layer_input, positions, norm_gain_attn, w_query, key_weight, value_weight, w_out, norm_gain_ffn, w_gate, w_up, w_down, out_cotangent):
    overall_accumulator = layer_input.shape[0]
    head_group = QUERY_HEADS // SHARED_KV_UNITS
    scale = 1.0 / math.sqrt(CHANNEL_SPAN)
    resid_in = layer_input.astype(jnp.float32)
    inverse_one = lax.rsqrt(lax.optimization_barrier(jnp.mean(resid_in * resid_in, axis=-1, keepdims=True)) + epsilon)
    normed_one = resid_in * inverse_one
    attention_normed = (normed_one * norm_gain_attn).astype(jnp.bfloat16)
    cosine_table, sine_table = rope_tables(positions)
    query_matrix = apply_rotary(jnp.dot(attention_normed, w_query, preferred_element_type=jnp.float32).reshape(overall_accumulator, QUERY_HEADS, CHANNEL_SPAN), cosine_table, sine_table).astype(jnp.bfloat16)
    key_matrix = apply_rotary(jnp.dot(attention_normed, key_weight, preferred_element_type=jnp.float32).reshape(overall_accumulator, SHARED_KV_UNITS, CHANNEL_SPAN), cosine_table, sine_table).astype(jnp.bfloat16)
    value_matrix = jnp.dot(attention_normed, value_weight, preferred_element_type=jnp.float32).astype(jnp.bfloat16)
    keys_wide = key_matrix.astype(jnp.float32)
    expanded_values = value_matrix.astype(jnp.float32).reshape(overall_accumulator, SHARED_KV_UNITS, CHANNEL_SPAN)
    rows_per_block = math.gcd(overall_accumulator, 128)
    block_list = overall_accumulator // rows_per_block
    query_block_list = query_matrix.reshape(block_list, rows_per_block, SHARED_KV_UNITS, head_group, CHANNEL_SPAN)
    position_blocks = positions.reshape(block_list, rows_per_block)

    def masked_scores(query_block, query_pos):
        scores = jnp.einsum('tgjd,sgd->gjts', query_block.astype(jnp.float32), keys_wide) * scale
        allowed = positions[None, :] <= query_pos[:, None]
        return jnp.where(allowed[None, None], scores, mask_fill_value)

    def forward_block(carry, item):
        query_block, query_pos = item
        scores = masked_scores(query_block, query_pos)
        largest = lax.optimization_barrier(jnp.max(scores, axis=-1))
        log_total = largest + jnp.log(lax.optimization_barrier(jnp.sum(jnp.exp(scores - largest[..., None]), axis=-1)))
        weights = rounded_copy(jnp.exp(scores - log_total[..., None]))
        mixed = jnp.einsum('gjts,sgd->tgjd', weights, expanded_values)
        return (carry, (mixed.astype(jnp.bfloat16), log_total))
    unused, (mixed_blocks, log_blocks) = lax.scan(forward_block, jnp.zeros((), jnp.float32), (query_block_list, position_blocks))
    attention_output = mixed_blocks.reshape(overall_accumulator, QUERY_HEADS * CHANNEL_SPAN)
    resid_mid = resid_in + jnp.dot(attention_output, w_out, preferred_element_type=jnp.float32)
    inverse_two = lax.rsqrt(lax.optimization_barrier(jnp.mean(resid_mid * resid_mid, axis=-1, keepdims=True)) + epsilon)
    normed_two = resid_mid * inverse_two
    normed_ffn = (normed_two * norm_gain_ffn).astype(jnp.bfloat16)
    gate = jnp.dot(normed_ffn, w_gate, preferred_element_type=jnp.float32)
    upward = jnp.dot(normed_ffn, w_up, preferred_element_type=jnp.float32)
    sigmoid = jax.nn.sigmoid(gate)
    swish = gate * sigmoid
    hidden = (swish * upward).astype(jnp.bfloat16)
    layer_output = (resid_mid + jnp.dot(hidden, w_down, preferred_element_type=jnp.float32)).astype(jnp.bfloat16)
    grad_down = weight_grad(hidden, out_cotangent)
    grad_hidden = back_project(out_cotangent, w_down)
    grad_gate_act = (grad_hidden * upward * sigmoid * (1.0 + gate * (1.0 - sigmoid))).astype(jnp.bfloat16)
    grad_up_act = (grad_hidden * swish).astype(jnp.bfloat16)
    grad_gate = weight_grad(normed_ffn, grad_gate_act)
    grad_up = weight_grad(normed_ffn, grad_up_act)
    grad_normed_two = back_project(grad_gate_act, w_gate) + back_project(grad_up_act, w_up)
    grad_resid_part, grad_norm_ffn = rms_backward(grad_normed_two, normed_two, inverse_two, norm_gain_ffn)
    grad_resid_mid = out_cotangent.astype(jnp.float32) + grad_resid_part
    grad_mid_low = grad_resid_mid.astype(jnp.bfloat16)
    grad_out = weight_grad(attention_output, grad_mid_low)
    attention_gradient = back_project(grad_mid_low, w_out).astype(jnp.bfloat16)
    delta_row_values = lax.optimization_barrier(jnp.sum((attention_gradient.astype(jnp.float32) * attention_output.astype(jnp.float32)).reshape(overall_accumulator, SHARED_KV_UNITS, head_group, CHANNEL_SPAN), axis=-1))
    block_gradients = attention_gradient.reshape(block_list, rows_per_block, SHARED_KV_UNITS, head_group, CHANNEL_SPAN)
    delta_block_list = delta_row_values.reshape(block_list, rows_per_block, SHARED_KV_UNITS, head_group)

    def backward_block(carry, item):
        key_gradient_sum, value_gradient_sum = carry
        query_block, query_pos, grad_block, log_total, delta_block = item
        scores = masked_scores(query_block, query_pos)
        weights = jnp.exp(scores - log_total[..., None])
        grad_wide = grad_block.astype(jnp.float32)
        value_gradient_sum = value_gradient_sum + jnp.einsum('gjts,tgjd->sgd', rounded_copy(weights), grad_wide)
        grad_weights = jnp.einsum('tgjd,sgd->gjts', grad_wide, expanded_values)
        grad_scores = rounded_copy(weights * (grad_weights - jnp.transpose(delta_block, (1, 2, 0))[..., None]))
        grad_query_block = jnp.einsum('gjts,sgd->tgjd', grad_scores, keys_wide) * scale
        key_gradient_sum = key_gradient_sum + jnp.einsum('gjts,tgjd->sgd', grad_scores, query_block.astype(jnp.float32)) * scale
        return ((key_gradient_sum, value_gradient_sum), grad_query_block)
    empty_sum = jnp.zeros((overall_accumulator, SHARED_KV_UNITS, CHANNEL_SPAN), jnp.float32)
    (key_gradient_sum, value_gradient_sum), grad_query_blocks = lax.scan(backward_block, (empty_sum, empty_sum), (query_block_list, position_blocks, block_gradients, log_blocks, delta_block_list))
    grad_queries = apply_rotary(grad_query_blocks.reshape(overall_accumulator, QUERY_HEADS, CHANNEL_SPAN), cosine_table, -sine_table).astype(jnp.bfloat16).reshape(overall_accumulator, QUERY_HEADS * CHANNEL_SPAN)
    key_gradients = apply_rotary(key_gradient_sum, cosine_table, -sine_table).astype(jnp.bfloat16).reshape(overall_accumulator, SHARED_KV_UNITS * CHANNEL_SPAN)
    value_gradients = value_gradient_sum.astype(jnp.bfloat16).reshape(overall_accumulator, SHARED_KV_UNITS * CHANNEL_SPAN)
    grad_query = weight_grad(attention_normed, grad_queries)
    grad_key = weight_grad(attention_normed, key_gradients)
    grad_value = weight_grad(attention_normed, value_gradients)
    grad_normed_one = back_project(grad_queries, w_query) + back_project(key_gradients, key_weight) + back_project(value_gradients, value_weight)
    grad_resid_in, grad_norm_attn = rms_backward(grad_normed_one, normed_one, inverse_one, norm_gain_attn)
    input_grad = (grad_resid_mid + grad_resid_in).astype(jnp.bfloat16)
    return (layer_output, input_grad, grad_norm_attn, grad_query, grad_key, grad_value, grad_out, grad_norm_ffn, grad_gate, grad_up, grad_down)
```

```python
import functools
import math

import jax
import jax.numpy as jnp
from jax import lax
from jax.experimental import pallas as pl
from jax.experimental.pallas import tpu as pltpu
from jax.sharding import PartitionSpec as P

HEAD = 96
GROUP = 2
EPSILON = 1e-05
ROPE_BASE = 100000.0
LOG2E = math.log2(math.e)
F32 = jnp.float32
BF16 = jnp.bfloat16

NN = (((1,), (0,)), ((), ()))
NT = (((1,), (1,)), ((), ()))
TN = (((0,), (0,)), ((), ()))
TT = (((0,), (1,)), ((), ()))


def dot(a, b, dims):
    return lax.dot_general(a, b, dims, preferred_element_type=F32)


def load_queries(q_ref, qs, blk):
    for part in range(2):
        lanes = slice(part * blk, (part + 1) * blk)
        qs[part] = jnp.concatenate([q_ref[0, j, :, lanes] for j in range(GROUP)], axis=1)


def causal_mask(blk):
    key_row = lax.broadcasted_iota(jnp.int32, (blk, GROUP * blk), 0)
    query_row = lax.broadcasted_iota(jnp.int32, (blk, GROUP * blk), 1) % blk
    return key_row <= query_row


def attention_forward(n, blk, unroll, info, q_ref, kv_ref, o_ref, lse_ref, qs, sc, mx, ls, acc):
    own = info[n]
    mine = info[own]
    factor = LOG2E / math.sqrt(HEAD)
    load_queries(q_ref, qs, blk)
    allowed = causal_mask(blk)

    def fold(value):
        return jnp.max(value, axis=0, keepdims=True)

    def product(c, lane, part):
        keys = kv_ref[c, 0, 0, :, pl.ds(lane, blk)]
        return dot(keys, qs[part], TN)

    diag_a = jnp.where(allowed, product(own, 0, 0), -1e30)
    full_b = product(own, 0, 1)
    diag_b = jnp.where(allowed, product(own, blk, 1), -1e30)
    sc[0], sc[1], sc[2] = diag_a, full_b, diag_b
    mx[0] = fold(diag_a)
    mx[1] = jnp.maximum(fold(full_b), fold(diag_b))

    def other(i):
        c = lax.rem(own + i, n)
        part = jnp.where(info[c] < mine, 0, 1)
        return c, part, pl.multiple_of(part * blk, blk)

    def score_step(i, carry):
        c, part, lane = other(i)
        first = product(c, 0, 1)
        second = product(c, lane, part)
        sc[2 * i + 1] = first
        sc[2 * i + 2] = second
        mx[1] = jnp.maximum(mx[1], fold(first))
        mx[part] = jnp.maximum(mx[part], fold(second))
        return carry

    lax.fori_loop(1, n, score_step, 0, unroll=unroll)
    mx[...] = mx[...] * factor

    def weigh(slot, c, lane, part):
        weights = jnp.exp2(sc[slot] * factor - mx[part])
        values = kv_ref[c, 1, 0, :, pl.ds(lane, blk)]
        return jnp.sum(weights, axis=0, keepdims=True), dot(values, weights.astype(BF16), NN)

    ls[0], acc[0] = weigh(0, own, 0, 0)
    sum_one, mix_one = weigh(1, own, 0, 1)
    sum_two, mix_two = weigh(2, own, blk, 1)
    ls[1] = sum_one + sum_two
    acc[1] = mix_one + mix_two

    def mix_step(i, carry):
        c, part, lane = other(i)
        total, mixed = weigh(2 * i + 1, c, 0, 1)
        ls[1] += total
        acc[1] += mixed
        total, mixed = weigh(2 * i + 2, c, lane, part)
        ls[part] += total
        acc[part] += mixed
        return carry

    lax.fori_loop(1, n, mix_step, 0, unroll=unroll)
    for part in range(2):
        lanes = slice(part * blk, (part + 1) * blk)
        mixed = (acc[part] / ls[part]).astype(BF16)
        total = mx[part] + jnp.log2(ls[part])
        for j in range(GROUP):
            o_ref[0, j, :, lanes] = mixed[:, j * blk : (j + 1) * blk]
            lse_ref[0, j : j + 1, lanes] = total[:, j * blk : (j + 1) * blk]


def attention_backward(
    n, blk, unroll, info, q_ref, g_ref, o_ref, lse_ref, kv_ref, dq_ref, dkv_ref, qs, gs, st, acc
):
    own = info[n]
    mine = info[own]
    scale = 1.0 / math.sqrt(HEAD)
    factor = LOG2E * scale
    load_queries(q_ref, qs, blk)
    load_queries(g_ref, gs, blk)
    allowed = causal_mask(blk)
    for part in range(2):
        lanes = slice(part * blk, (part + 1) * blk)
        for j in range(GROUP):
            cols = slice(j * blk, (j + 1) * blk)
            st[part, 0:1, cols] = lse_ref[0, j : j + 1, lanes]
            st[part, 1:2, cols] = jnp.sum(
                g_ref[0, j, :, lanes].astype(F32) * o_ref[0, j, :, lanes].astype(F32),
                axis=0,
                keepdims=True,
            )

    def product(c, lane, part, masked=False):
        keys = kv_ref[c, 0, 0, :, pl.ds(lane, blk)]
        values = kv_ref[c, 1, 0, :, pl.ds(lane, blk)]
        queries = qs[part]
        grads = gs[part]
        weights = jnp.exp2(dot(keys, queries, TN) * factor - st[part, 0:1])
        if masked:
            weights = jnp.where(allowed, weights, 0.0)
        slope = (weights * (dot(values, grads, TN) - st[part, 1:2])).astype(BF16)
        return (
            dot(queries, slope, NT),
            dot(grads, weights.astype(BF16), NT),
            dot(keys, slope, NN),
        )

    key_a, value_a, acc[0] = product(own, 0, 0, True)
    key_b, value_b, query_b = product(own, 0, 1)
    key_c, value_c, query_c = product(own, blk, 1, True)
    acc[1] = query_b + query_c
    dkv_ref[own, 0, 0, :, 0:blk] = ((key_a + key_b) * scale).astype(BF16)
    dkv_ref[own, 1, 0, :, 0:blk] = (value_a + value_b).astype(BF16)
    dkv_ref[own, 0, 0, :, blk : 2 * blk] = (key_c * scale).astype(BF16)
    dkv_ref[own, 1, 0, :, blk : 2 * blk] = value_c.astype(BF16)

    def step(i, carry):
        c = lax.rem(own + i, n)
        part = jnp.where(info[c] < mine, 0, 1)
        lane = pl.multiple_of(part * blk, blk)
        key_one, value_one, query_one = product(c, 0, 1)
        key_two, value_two, query_two = product(c, lane, part)
        acc[1] += query_one
        acc[part] += query_two
        late = part == 1
        dkv_ref[c, 0, 0, :, 0:blk] = (
            (key_one + jnp.where(late, 0.0, key_two)) * scale
        ).astype(BF16)
        dkv_ref[c, 1, 0, :, 0:blk] = (value_one + jnp.where(late, 0.0, value_two)).astype(BF16)
        dkv_ref[c, 0, 0, :, blk : 2 * blk] = (jnp.where(late, key_two, 0.0) * scale).astype(BF16)
        dkv_ref[c, 1, 0, :, blk : 2 * blk] = jnp.where(late, value_two, 0.0).astype(BF16)
        return carry

    lax.fori_loop(1, n, step, 0, unroll=unroll)
    for part in range(2):
        lanes = slice(part * blk, (part + 1) * blk)
        total = acc[part] * scale
        for j in range(GROUP):
            dq_ref[0, j, :, lanes] = total[:, j * blk : (j + 1) * blk]


def unroll_of(n):
    return 3 if (n - 1) % 3 == 0 else 1


def run_forward(info, queries, kv, n, blk):
    heads = kv.shape[2]
    head_spec = pl.BlockSpec((1, GROUP, HEAD, 2 * blk), lambda g, *_: (g, 0, 0, 0))
    kv_spec = pl.BlockSpec((n, 2, 1, HEAD, 2 * blk), lambda g, *_: (0, 0, g, 0, 0))
    stat_spec = pl.BlockSpec((1, GROUP, 2 * blk), lambda g, *_: (g, 0, 0))
    pairs = heads * GROUP * 33 * blk * blk
    return pl.pallas_call(
        functools.partial(attention_forward, n, blk, unroll_of(n)),
        grid_spec=pltpu.PrefetchScalarGridSpec(
            num_scalar_prefetch=1,
            grid=(heads,),
            in_specs=[head_spec, kv_spec],
            out_specs=[head_spec, stat_spec],
            scratch_shapes=[
                pltpu.VMEM((2, HEAD, GROUP * blk), BF16),
                pltpu.VMEM((2 * n + 1, blk, GROUP * blk), F32),
                pltpu.VMEM((2, 1, GROUP * blk), F32),
                pltpu.VMEM((2, 1, GROUP * blk), F32),
                pltpu.VMEM((2, HEAD, GROUP * blk), F32),
            ],
        ),
        out_shape=[
            jax.ShapeDtypeStruct((heads, GROUP, HEAD, 2 * blk), BF16),
            jax.ShapeDtypeStruct((heads, GROUP, 2 * blk), F32),
        ],
        cost_estimate=pl.CostEstimate(
            flops=4 * HEAD * pairs, bytes_accessed=kv.size * 2, transcendentals=pairs
        ),
        name="attend",
    )(info, queries, kv)


def run_backward(info, queries, grads, outputs, stats, kv, n, blk):
    heads = kv.shape[2]
    head_spec = pl.BlockSpec((1, GROUP, HEAD, 2 * blk), lambda g, *_: (g, 0, 0, 0))
    kv_spec = pl.BlockSpec((n, 2, 1, HEAD, 2 * blk), lambda g, *_: (0, 0, g, 0, 0))
    stat_spec = pl.BlockSpec((1, GROUP, 2 * blk), lambda g, *_: (g, 0, 0))
    pairs = heads * GROUP * 33 * blk * blk
    return pl.pallas_call(
        functools.partial(attention_backward, n, blk, unroll_of(n)),
        grid_spec=pltpu.PrefetchScalarGridSpec(
            num_scalar_prefetch=1,
            grid=(heads,),
            in_specs=[head_spec, head_spec, head_spec, stat_spec, kv_spec],
            out_specs=[head_spec, kv_spec],
            scratch_shapes=[
                pltpu.VMEM((2, HEAD, GROUP * blk), BF16),
                pltpu.VMEM((2, HEAD, GROUP * blk), BF16),
                pltpu.VMEM((2, 2, GROUP * blk), F32),
                pltpu.VMEM((2, HEAD, GROUP * blk), F32),
            ],
        ),
        out_shape=[
            jax.ShapeDtypeStruct((heads, GROUP, HEAD, 2 * blk), F32),
            jax.ShapeDtypeStruct(kv.shape, BF16),
        ],
        cost_estimate=pl.CostEstimate(
            flops=10 * HEAD * pairs, bytes_accessed=kv.size * 4, transcendentals=pairs
        ),
        name="attend_back",
    )(info, queries, grads, outputs, stats, kv)


def rotate(value, cosine, sine):
    half = HEAD // 2
    first, second = value[:, :half], value[:, half:]
    return jnp.concatenate(
        [first * cosine - second * sine, second * cosine + first * sine], axis=1
    )


def rms(value):
    return lax.rsqrt(jnp.mean(value * value, axis=-1, keepdims=True) + EPSILON)


def rms_backward(grad, normed, inverse, gain):
    scaled = grad * gain
    inner = jnp.mean(scaled * normed, axis=-1, keepdims=True)
    return inverse * (scaled - normed * inner)


def body(
    n,
    layer_input,
    positions,
    norm_gain_attn,
    w_query,
    key_weight,
    value_weight,
    w_out,
    norm_gain_ffn,
    w_gate,
    w_up,
    w_down,
    out_cotangent,
):
    c = lax.axis_index("ctx")
    s = lax.axis_index("shard")
    o = 1 - s
    core = lax.rem(c, 2)
    rows, width = layer_input.shape
    half = rows // 2
    blk = 2 * half
    pair_rows = 2 * rows

    def swap(value):
        return lax.ppermute(value, "shard", [(0, 1), (1, 0)])

    def core_swap(value):
        return lax.ppermute(value, "ctx", [(i, i ^ 1) for i in range(n)])

    def columns(weight, index):
        size = weight.shape[1] // 2
        return lax.dynamic_slice_in_dim(weight, index * size, size, 1)

    def gather_columns(*weights):
        k = weights[0].shape[0]
        q = k // 2
        own = jnp.concatenate([columns(w, s) for w in weights], axis=1)
        send = jnp.concatenate(
            [columns(lax.dynamic_slice_in_dim(w, core * q, q, 0), o) for w in weights], axis=1
        )
        near = swap(send)
        far = core_swap(near)
        whole = jnp.zeros((2 * k, own.shape[1]), own.dtype)
        whole = lax.dynamic_update_slice_in_dim(whole, own, s * k, 0)
        whole = lax.dynamic_update_slice_in_dim(whole, near, o * k + core * q, 0)
        return lax.dynamic_update_slice_in_dim(whole, far, o * k + (1 - core) * q, 0)

    def join(own, other):
        own = own.reshape(2, 1, half, -1)
        other = other.reshape(2, 1, half, -1)
        first = jnp.where(s == 0, own, other)
        second = jnp.where(s == 0, other, own)
        return jnp.concatenate([first, second], axis=1).reshape(pair_rows, -1)

    def mine(value):
        value = value.reshape(2, 2, half, -1)
        return lax.dynamic_index_in_dim(value, s, 1, False).reshape(rows, -1)

    def theirs(value):
        value = value.reshape(2, 2, half, -1)
        return lax.dynamic_index_in_dim(value, o, 1, False).reshape(rows, -1)

    resid_in = join(layer_input, swap(layer_input)).astype(F32)
    w_qkv = gather_columns(w_query, key_weight, value_weight)
    cotangent = join(out_cotangent, swap(out_cotangent))
    wg = gather_columns(w_gate)
    wu = gather_columns(w_up)

    numbers = positions.reshape(n, pair_rows)[:, 0] // blk
    info = jnp.concatenate([numbers, c[None]]).astype(jnp.int32)
    pair_positions = lax.dynamic_index_in_dim(
        positions.reshape(n, 2, 2, half), c, 0, False
    ).transpose(1, 0, 2).reshape(pair_rows)
    frequency = ROPE_BASE ** (-2.0 * jnp.arange(HEAD // 2, dtype=F32) / HEAD)
    angles = frequency[:, None] * pair_positions.astype(F32)[None, :]
    cosine, sine = jnp.cos(angles), jnp.sin(angles)

    inverse_one = rms(resid_in)
    normed_one = resid_in * inverse_one
    attn_in = (normed_one * norm_gain_attn).astype(BF16)
    q_half = w_query.shape[1] // 2
    kv_half = key_weight.shape[1] // 2
    heads = kv_half // HEAD
    qkv = dot(w_qkv, attn_in, TT)
    queries = rotate(qkv[:q_half].reshape(-1, HEAD, pair_rows), cosine, sine)
    keys = rotate(qkv[q_half : q_half + kv_half].reshape(-1, HEAD, pair_rows), cosine, sine)
    values = qkv[q_half + kv_half :].reshape(-1, HEAD, pair_rows)
    queries = queries.astype(BF16).reshape(heads, GROUP, HEAD, pair_rows)
    kv_own = jnp.stack([keys, values]).astype(BF16)
    kv = lax.all_gather(kv_own.reshape(2 * kv_half, pair_rows), "ctx").reshape(
        n, 2, heads, HEAD, pair_rows
    )
    attention, stats = run_forward(info, queries, kv, n, blk)
    attention_flat = attention.reshape(q_half, pair_rows)

    partial = dot(attention_flat, w_out, TN).astype(BF16)
    resid_mid = resid_in + (partial.astype(F32) + swap(partial).astype(F32))
    inverse_two = rms(resid_mid)
    normed_two = resid_mid * inverse_two
    ffn_in = (normed_two * norm_gain_ffn).astype(BF16)
    gate = dot(ffn_in, wg, NN)
    upward = dot(ffn_in, wu, NN)
    sigmoid = jax.nn.sigmoid(gate)
    swish = gate * sigmoid
    hidden = (swish * upward).astype(BF16)
    down = dot(hidden, w_down, NN)
    layer_output = (
        mine(resid_mid) + mine(down) + swap(theirs(down).astype(BF16)).astype(F32)
    ).astype(BF16)

    grad_hidden = dot(cotangent, w_down, NT)
    grad_gate_act = (grad_hidden * upward * sigmoid * (1.0 + gate * (1.0 - sigmoid))).astype(BF16)
    grad_up_act = (grad_hidden * swish).astype(BF16)
    partial = (dot(grad_gate_act, wg, NT) + dot(grad_up_act, wu, NT)).astype(BF16)
    grad_normed_two = partial.astype(F32) + swap(partial).astype(F32)
    grad_resid_mid = cotangent.astype(F32) + rms_backward(
        grad_normed_two, normed_two, inverse_two, norm_gain_ffn
    )
    gain_ffn = jnp.sum(mine(grad_normed_two * normed_two), axis=0)
    grad_mid_low = grad_resid_mid.astype(BF16)
    grad_attention = dot(w_out, grad_mid_low, NT).astype(BF16)

    def scatter(value):
        value = value.astype(BF16).reshape(n, value.shape[0] // n, -1)
        return lax.psum_scatter(value, "ctx", scatter_dimension=0, tiled=False)

    def spread_columns(value):
        r = value.shape[0] // 2
        own = lax.dynamic_slice_in_dim(value, s * r, r, 0)
        other = swap(lax.dynamic_slice_in_dim(value, o * r, r, 0))
        first = jnp.where(s == 0, own, other)
        second = jnp.where(s == 0, other, own)
        return jnp.concatenate([first, second], axis=1).astype(F32)

    def spread_rows(value):
        moves = [(2 * i + j, n * j + i) for i in range(n) for j in range(2)]
        return lax.ppermute(value, ("ctx", "shard"), moves).astype(F32)

    grad_down = spread_rows(scatter(dot(hidden, cotangent, TN)))
    grad_gate = spread_columns(scatter(dot(ffn_in, grad_gate_act, TN)))
    grad_up = spread_columns(scatter(dot(ffn_in, grad_up_act, TN)))
    grad_out = spread_rows(scatter(dot(attention_flat, grad_mid_low, NN)))

    grad_query_t, grad_kv = run_backward(
        info,
        queries,
        grad_attention.reshape(queries.shape),
        attention,
        stats,
        kv,
        n,
        blk,
    )
    grad_kv = lax.psum_scatter(
        grad_kv.reshape(n, 2 * kv_half, pair_rows), "ctx", scatter_dimension=0, tiled=False
    ).astype(F32)
    grad_queries = rotate(grad_query_t.reshape(-1, HEAD, pair_rows), cosine, -sine)
    grad_keys = rotate(grad_kv[:kv_half].reshape(-1, HEAD, pair_rows), cosine, -sine)
    grad_qkv = jnp.concatenate(
        [
            grad_queries.reshape(q_half, pair_rows),
            grad_keys.reshape(kv_half, pair_rows),
            grad_kv[kv_half:],
        ]
    ).astype(BF16)
    partial = dot(grad_qkv, w_qkv, TT)
    grad_normed_one = mine(partial) + swap(theirs(partial).astype(BF16)).astype(F32)
    normed_own = mine(normed_one)
    grad_resid_in = rms_backward(grad_normed_one, normed_own, mine(inverse_one), norm_gain_attn)
    gain_attn = jnp.sum(grad_normed_one * normed_own, axis=0)
    input_grad = (mine(grad_resid_mid) + grad_resid_in).astype(BF16)

    local = scatter(dot(attn_in, grad_qkv, TT))
    grad_query = spread_columns(local[:, :q_half])
    grad_key = spread_columns(local[:, q_half : q_half + kv_half])
    grad_value = spread_columns(local[:, q_half + kv_half :])

    gains = jnp.stack([gain_attn.reshape(2 * n, -1), gain_ffn.reshape(2 * n, -1)], axis=1)
    gains = lax.psum_scatter(gains, ("ctx", "shard"), scatter_dimension=0, tiled=False)
    return (
        layer_output,
        input_grad,
        gains[0],
        grad_query,
        grad_key,
        grad_value,
        grad_out,
        gains[1],
        grad_gate,
        grad_up,
        grad_down,
    )


def solution(mesh):
    both = P(("ctx", "shard"), None)
    shard = P("shard", None)
    vector = P(("ctx", "shard"))
    return jax.shard_map(
        functools.partial(body, mesh.shape["ctx"]),
        mesh=mesh,
        in_specs=(both, P(), P(), shard, shard, shard, shard, P(), shard, shard, shard, both),
        out_specs=(both, both, vector, both, both, both, both, vector, both, both, both),
        check_vma=False,
    )
```
